128 devices in a mesh: outer: 8 (over x, z_hi), inner: 16 (over z_lo, y, core).
Axes of the slice: x: 4, y: 4, z: 4 (z_hi: 2, z_lo: 2; z = z_hi * 2 + z_lo), core: 2. Of those that a mesh axis runs over, the one named last changes fastest.
Arguments:
- queries: bfloat16 [16384, 4096], P(('outer', 'inner')), may hold values from -24 to 24, as said below
- keys: bfloat16 [16384, 1024], P(('outer', 'inner')), may hold values from -24 to 24, as said below
- values: bfloat16 [16384, 1024], P(('outer', 'inner')), may hold values from -6 to 6
Outputs:
- attended: bfloat16 [16384, 4096], P(('outer', 'inner'))
The draws below stay inside these ranges and needn't reach their ends.
Inputs may be any that keep to these rules, and one draw needn't show every extreme that they name: `queries`: entries of order one, a few larger. `keys`: entries of order one, a few larger.
All inputs are finite; a program needn't handle non-finite values.
Results may differ from the reference program's by a relative error of at most 0.008.
Values may be sent and summed in bfloat16 or wider, within the bound.
A program may use at most 128 MiB of HBM per device.

```python
import jax
import jax.numpy as jnp
from jax import lax

QH = 32
KVH = 8
HD = 128
TOK_DEV = 128
TOKENS = 16384
N_OUTER = 8
N_INNER = 16


def shared_fields(key):
    base = jax.random.fold_in(key, 11)
    ratio = QH // KVH
    key_noise = jnp.clip(jax.random.normal(jax.random.fold_in(base, 1), (TOKENS, KVH, HD), jnp.float32), -6.0, 6.0)
    query_noise = jnp.clip(jax.random.normal(jax.random.fold_in(base, 2), (TOKENS, KVH, ratio, HD), jnp.float32), -6.0, 6.0)
    key_noise = jnp.clip(key_noise, -24.0, 24.0)
    query_noise = jnp.clip(query_noise, -24.0, 24.0)
    return (query_noise, key_noise)


def draw_queries(key, part):
    query_noise, key_noise = shared_fields(key)
    return query_noise.reshape(TOKENS, QH * HD).astype(jnp.bfloat16)


def draw_keys(key, part):
    query_noise, key_noise = shared_fields(key)
    return key_noise.reshape(TOKENS, KVH * HD).astype(jnp.bfloat16)


def shard_levels(rng, shape, shards, smallest, top_value):
    def one(dim, shards_of):
        heights = jax.random.uniform(jax.random.fold_in(jax.random.fold_in(rng, 6), dim), (shards_of,), jnp.float32, smallest / len(shards), top_value / len(shards))
        return jnp.repeat(jnp.exp(heights), shape[dim] // shards_of).reshape((-1,) + (1,) * (len(shape) - dim - 1))

    factor_of = one(*shards[0])
    for cut in shards[1:]:
        factor_of = factor_of * one(*cut)
    return factor_of


def gaussian(stream_key, dims, scale, bound, split=(), held_as=jnp.bfloat16):
    values = scale * jax.random.normal(stream_key, dims, jnp.float32)
    if split:
        values = values * shard_levels(stream_key, dims, split, -0.22, 0.18)
    return jnp.clip(values, -bound, bound).astype(held_as)


def setup_inputs(seed: int = 0) -> dict:
    key_of = jax.random.split(jax.random.key(seed), 4)
    queries = draw_queries(jax.random.fold_in(key_of[3], 71), 0)
    keys = draw_keys(jax.random.fold_in(key_of[3], 71), 0)
    values = gaussian(key_of[2], (TOKENS, KVH * HD), 1.0, 6.0, ((0, 128),))
    return dict(queries=queries, keys=keys, values=values)


def reference(queries, keys, values):
    group = TOK_DEV * N_INNER
    length = group * N_OUTER
    ratio = QH // KVH
    scale = 1.0 / (HD ** 0.5)
    padded_keys = jnp.pad(keys.reshape(length, KVH, HD), ((group, group), (0, 0), (0, 0)))
    padded_values = jnp.pad(values.reshape(length, KVH, HD), ((group, group), (0, 0), (0, 0)))
    block = 256 if group % 256 == 0 else group
    blocks = length // block

    def one_block(index):
        start = (index * block).astype(jnp.int32)
        owner = (start // group).astype(jnp.int32)
        rows = lax.dynamic_slice_in_dim(queries, start, block, 0)
        rows = rows.reshape(block, KVH, ratio, HD).astype(jnp.float32)
        near_keys = lax.dynamic_slice_in_dim(padded_keys, (owner * group).astype(jnp.int32), 3 * group, 0).astype(jnp.float32)
        near_values = lax.dynamic_slice_in_dim(padded_values, (owner * group).astype(jnp.int32), 3 * group, 0).astype(jnp.float32)
        scores = jnp.einsum("qgrd,kgd->grqk", rows, near_keys) * scale
        source = owner - 1 + (jnp.arange(3 * group, dtype=jnp.int32) // group)
        inside = (source >= 0) & (source < N_OUTER)
        scores = jnp.where(inside, scores, -jnp.inf)
        peak = jnp.max(scores, axis=-1, keepdims=True)
        weights = jnp.exp(scores - peak)
        total = jnp.sum(weights, axis=-1)
        rounded = weights.astype(jnp.bfloat16).astype(jnp.float32)
        mixed = jnp.einsum("grqk,kgd->grqd", rounded, near_values) / total[..., None]
        return mixed.transpose(2, 0, 1, 3).reshape(block, QH * HD).astype(jnp.bfloat16)

    result = lax.map(one_block, jnp.arange(blocks, dtype=jnp.int32))
    return result.reshape(length, QH * HD)
```

```python
import jax
import jax.numpy as jnp
from jax import lax
from jax.experimental import pallas as pl
from jax.experimental.pallas import tpu as pltpu
from jax.sharding import PartitionSpec as P

QH = 32
KVH = 8
HD = 128
TOK = 128
RATIO = QH // KVH
ROWS = RATIO * TOK
HALF = 8 * TOK
SEG = 2 * HALF
KT = 256
SCALE = 1.4426950408889634 / HD**0.5
MESH = pl.DeviceIdType.MESH


def rotation(slot):
    turn = slot // 2
    return turn + (turn // 2) * (5 - 2 * turn), slot % 2


def mirrored(slot):
    turn = slot // 2
    return 2 * ((2 * turn) % 3 + 3 * (turn // 3)) + slot % 2


def kernel(
    q_hbm, k_hbm, v_hbm, o_hbm,
    q_buf, k_buf, v_buf, o_buf, s_buf, m_cur, m_run, acc,
    q_out, q_in, kv_out, kv_in, sib_out, sib_in, hop_out, hop_in, o_out, o_in,
):
    outer = lax.axis_index("outer")
    inner = lax.axis_index("inner")
    z_hi = outer % 2
    z_lo = inner // 8
    y = (inner // 2) % 4
    core = inner % 2

    def peer(slot):
        dy, dz = rotation(slot)
        py = (y + dy) % 4
        pz = (z_lo + dz) % 2
        head = ((pz + z_hi) % 2) * 4 + py
        return (outer, pz * 8 + py * 2 + core), head

    def columns(head, width):
        return pl.ds(pl.multiple_of(head * width, width), width)

    my_head = ((z_lo + z_hi) % 2) * 4 + y
    sibling = (outer, inner + 1 - 2 * core)
    across = (1 - z_lo) * 8 + y * 2 + core
    near = (outer + 1 - 2 * z_hi, across)
    far_outer = outer - 1 + 2 * z_hi
    far = (far_outer, across)
    has_far = jnp.logical_and(far_outer >= 0, far_outer < 8)
    no_far = jnp.logical_not(has_far)

    barrier = pltpu.get_barrier_semaphore()

    def greet(device):
        pl.semaphore_signal(barrier, inc=1, device_id=device, device_id_type=MESH)

    for slot in range(1, 8):
        greet(peer(slot)[0])
    greet(sibling)
    greet(near)

    @pl.when(has_far)
    def _():
        greet(far)
        pl.semaphore_wait(barrier, 10)

    @pl.when(no_far)
    def _():
        pl.semaphore_wait(barrier, 9)

    def remote(src, dst, send, recv, device):
        return pltpu.make_async_remote_copy(
            src_ref=src, dst_ref=dst, send_sem=send, recv_sem=recv,
            device_id=device, device_id_type=MESH,
        )

    def kv_copy(slot, which):
        device, head = peer(slot)
        back = mirrored(slot)
        hbm, buf = ((k_hbm, k_buf), (v_hbm, v_buf))[which]
        return remote(
            hbm.at[:, columns(head, HD)],
            buf.at[0, 0, pl.ds(back * TOK, TOK), :],
            kv_out.at[which, slot], kv_in.at[which, back], device,
        )

    def q_copy(slot):
        device, head = peer(slot)
        back = mirrored(slot)
        return remote(
            q_hbm.at[:, columns(head, RATIO * HD)],
            q_buf.at[back], q_out.at[slot], q_in.at[back], device,
        )

    def own_kv(which):
        hbm, buf = ((k_hbm, k_buf), (v_hbm, v_buf))[which]
        return pltpu.make_async_copy(
            hbm.at[:, columns(my_head, HD)],
            buf.at[0, 0, pl.ds(0, TOK), :], kv_in.at[which, 0],
        )

    own_q = pltpu.make_async_copy(
        q_hbm.at[:, columns(my_head, RATIO * HD)], q_buf.at[0], q_in.at[0]
    )

    for which in range(2):
        own_kv(which).start()
    for slot in range(1, 8):
        for which in range(2):
            kv_copy(slot, which).start()
    own_q.start()
    for slot in range(1, 8):
        q_copy(slot).start()

    def to_sibling(seg, which):
        buf = (k_buf, v_buf)[which]
        return remote(
            buf.at[seg, 0], buf.at[seg, 1],
            sib_out.at[seg, which], sib_in.at[seg, which], sibling,
        )

    def hop(seg, which):
        buf = (k_buf, v_buf)[which]
        return remote(
            buf.at[0, 0], buf.at[seg, 0],
            hop_out.at[seg - 1, which], hop_in.at[seg - 1, which],
            near if seg == 1 else far,
        )

    for which in range(2):
        own_kv(which).wait()
        for slot in range(1, 8):
            kv_copy(slot, which).wait_recv()
        to_sibling(0, which).start()
        hop(1, which).start()
    own_q.wait()

    def wait_q(slot):
        remote(
            q_hbm.at[:, columns(0, RATIO * HD)],
            q_buf.at[slot], q_out.at[slot], q_in.at[slot], sibling,
        ).wait_recv()

    def score(b, seg, side):
        q = jnp.concatenate(
            [q_buf[b, :, h * HD : (h + 1) * HD] for h in range(RATIO)], axis=0
        )
        for kt in range(SEG // KT):
            half, at = divmod(kt * KT, HALF)
            s_buf[side, :, kt * KT : (kt + 1) * KT] = lax.dot_general(
                q, k_buf[seg, half, at : at + KT, :],
                (((1,), (1,)), ((), ())), preferred_element_type=jnp.float32,
            )
        for h in range(RATIO):
            r = slice(h * TOK, (h + 1) * TOK)
            top = s_buf[side, r, 0:HD]
            for j in range(1, SEG // HD):
                top = jnp.maximum(top, s_buf[side, r, j * HD : (j + 1) * HD])
            top = jnp.broadcast_to(jnp.max(top, axis=1, keepdims=True), (TOK, HD))
            if seg:
                top = jnp.maximum(top, m_run[b, r, :])
            m_cur[side, r, :] = top

    def mix(b, seg, side):
        m = m_cur[side]
        update = None
        for kt in range(SEG // KT):
            half, at = divmod(kt * KT, HALF)
            p = jnp.concatenate(
                [
                    jnp.exp2((s_buf[side, :, c : c + HD] - m) * SCALE).astype(jnp.bfloat16)
                    for c in range(kt * KT, (kt + 1) * KT, HD)
                ],
                axis=1,
            )
            wide = jnp.concatenate(
                [v_buf[seg, half, at : at + KT, :], jnp.ones((KT, HD), jnp.bfloat16)], axis=1
            )
            part = jnp.dot(p, wide, preferred_element_type=jnp.float32)
            update = part if update is None else update + part
        if seg:
            factor = jnp.exp2((m_run[b] - m) * SCALE)
            update = acc[b] * jnp.concatenate([factor, factor], axis=1) + update
        if seg < 2:
            m_run[b] = m
            acc[b] = update
        else:
            finish(b, update)

    def finish(b, total):
        mixed = (total[:, :HD] / total[:, HD:]).astype(jnp.bfloat16)
        for h in range(RATIO):
            o_buf[b, :, h * HD : (h + 1) * HD] = mixed[h * TOK : (h + 1) * TOK, :]

    def give(b):
        device, head = peer(b)
        return remote(
            o_buf.at[b], o_hbm.at[:, columns(my_head, RATIO * HD)],
            o_out.at[b], o_in.at[mirrored(b)], device,
        )

    own_o = pltpu.make_async_copy(
        o_buf.at[0], o_hbm.at[:, columns(my_head, RATIO * HD)], o_in.at[0]
    )

    def send_out(b):
        @pl.when(b == 0)
        def _():
            own_o.start()

        @pl.when(b > 0)
        def _():
            give(b).start()

    for which in range(2):
        to_sibling(0, which).wait_recv()

    def phase(seg, before_last):
        score(0, seg, 0)

        def body(i, carry):
            b = 2 * i
            if seg == 0:
                wait_q(b + 1)
            if before_last is not None:
                pl.when(i == 3)(before_last)
            score(b + 1, seg, 1)
            mix(b, seg, 0)
            if seg == 0:

                @pl.when(i < 3)
                def _():
                    wait_q(b + 2)

            if seg == 2:
                send_out(b)
            score(jnp.minimum(b + 2, 7), seg, 0)
            mix(b + 1, seg, 1)
            if seg == 2:
                send_out(b + 1)
            return carry

        lax.fori_loop(0, 4, body, 0)

    def near_arrives():
        for which in range(2):
            hop(1, which).wait_recv()
            to_sibling(1, which).start()

        @pl.when(has_far)
        def _():
            for which in range(2):
                hop(2, which).start()

    def far_arrives():
        @pl.when(has_far)
        def _():
            for which in range(2):
                hop(2, which).wait_recv()
                to_sibling(2, which).start()

    phase(0, near_arrives)
    for which in range(2):
        to_sibling(1, which).wait_recv()
    phase(1, far_arrives)

    @pl.when(has_far)
    def _():
        for which in range(2):
            to_sibling(2, which).wait_recv()
        phase(2, None)

    @pl.when(no_far)
    def _():
        def body(b, carry):
            finish(b, acc[b])
            send_out(b)
            return carry

        lax.fori_loop(0, 8, body, 0)

    for slot in range(1, 8):
        for which in range(2):
            kv_copy(slot, which).wait_send()
        q_copy(slot).wait_send()
    for which in range(2):
        to_sibling(0, which).wait_send()
        to_sibling(1, which).wait_send()
        hop(1, which).wait_send()

    @pl.when(has_far)
    def _():
        for which in range(2):
            to_sibling(2, which).wait_send()
            hop(2, which).wait_send()

    own_o.wait()
    for slot in range(1, 8):
        device, head = peer(slot)
        give(slot).wait_send()
        remote(
            o_buf.at[slot], o_hbm.at[:, columns(head, RATIO * HD)],
            o_out.at[slot], o_in.at[slot], device,
        ).wait_recv()


def attention(queries, keys, values):
    dma = pltpu.SemaphoreType.DMA
    return pl.pallas_call(
        kernel,
        out_shape=jax.ShapeDtypeStruct(queries.shape, jnp.bfloat16),
        in_specs=[pl.BlockSpec(memory_space=pl.ANY)] * 3,
        out_specs=pl.BlockSpec(memory_space=pl.ANY),
        scratch_shapes=[
            pltpu.VMEM((8, TOK, RATIO * HD), jnp.bfloat16),
            pltpu.VMEM((3, 2, HALF, HD), jnp.bfloat16),
            pltpu.VMEM((3, 2, HALF, HD), jnp.bfloat16),
            pltpu.VMEM((8, TOK, RATIO * HD), jnp.bfloat16),
            pltpu.VMEM((2, ROWS, SEG), jnp.float32),
            pltpu.VMEM((2, ROWS, HD), jnp.float32),
            pltpu.VMEM((8, ROWS, HD), jnp.float32),
            pltpu.VMEM((8, ROWS, 2 * HD), jnp.float32),
            dma((8,)), dma((8,)),
            dma((2, 8)), dma((2, 8)),
            dma((3, 2)), dma((3, 2)),
            dma((2, 2)), dma((2, 2)),
            dma((8,)), dma((8,)),
        ],
        compiler_params=pltpu.CompilerParams(
            collective_id=0, has_side_effects=True, vmem_limit_bytes=58 * 2**20
        ),
        name="window_attention",
    )(queries, keys, values)


def solution(mesh):
    spec = P(("outer", "inner"), None)
    return jax.shard_map(
        attention, mesh=mesh, in_specs=(spec, spec, spec), out_specs=spec, check_vma=False
    )
```

```python
import jax
import jax.numpy as jnp
from jax import lax
from jax.experimental import pallas as pl
from jax.experimental.pallas import tpu as pltpu
from jax.sharding import PartitionSpec as P

QH = 32
KVH = 8
HD = 128
TOK = 128
RATIO = QH // KVH
ROWS = RATIO * TOK
HALF = 8 * TOK
SEG = 2 * HALF
KT = 256
SCALE = 1.4426950408889634 / HD**0.5
MESH = pl.DeviceIdType.MESH


STEPS = ((0, 0), (1, 0), (3, 0), (0, 1), (1, 1), (3, 1), (2, 0), (2, 1))
BACK = tuple(STEPS.index(((4 - dy) % 4, dz)) for dy, dz in STEPS)
CHUNKS = 4
CHUNK = HALF // CHUNKS


def kernel(
    q_hbm, k_hbm, v_hbm, o_hbm,
    q_buf, k_buf, v_buf, o_buf, s_buf, m_cur, m_run, acc,
    q_out, q_in, kv_out, kv_in, own_out, own_in, hop_out, hop_in,
    next_out, next_in, relay_out, relay_in, last_out, last_in, o_out, o_in,
):
    outer = lax.axis_index("outer")
    inner = lax.axis_index("inner")
    z_hi = outer % 2
    z_lo = inner // 8
    y = (inner // 2) % 4
    core = inner % 2
    kv = ((k_hbm, k_buf), (v_hbm, v_buf))

    def peer(slot):
        dy, dz = STEPS[slot]
        py = (y + dy) % 4
        pz = (z_lo + dz) % 2
        head = ((pz + z_hi) % 2) * 4 + py
        return (outer, pz * 8 + py * 2 + core), head

    def columns(head, width):
        return pl.ds(pl.multiple_of(head * width, width), width)

    my_head = ((z_lo + z_hi) % 2) * 4 + y
    sibling = (outer, inner + 1 - 2 * core)
    near = (outer + 1 - 2 * z_hi, (1 - z_lo) * 8 + y * 2 + core)
    onward_outer = outer + 2 - 4 * z_hi
    source_outer = outer - 2 + 4 * z_hi
    onward = (onward_outer, inner)
    source = (source_outer, inner)
    has_onward = jnp.logical_and(onward_outer >= 0, onward_outer < 8)
    has_far = jnp.logical_and(source_outer >= 0, source_outer < 8)
    no_far = jnp.logical_not(has_far)

    barrier = pltpu.get_barrier_semaphore()

    def greet(device):
        pl.semaphore_signal(barrier, inc=1, device_id=device, device_id_type=MESH)

    for slot in range(1, 8):
        greet(peer(slot)[0])
    greet(sibling)
    greet(near)

    @pl.when(has_onward)
    def _():
        greet(onward)

    @pl.when(has_far)
    def _():
        greet(source)

    inland = jnp.logical_and(has_onward, has_far)

    @pl.when(inland)
    def _():
        pl.semaphore_wait(barrier, 11)

    @pl.when(jnp.logical_not(inland))
    def _():
        pl.semaphore_wait(barrier, 10)

    def remote(src, dst, send, recv, device):
        return pltpu.make_async_remote_copy(
            src_ref=src, dst_ref=dst, send_sem=send, recv_sem=recv,
            device_id=device, device_id_type=MESH,
        )

    def kv_copy(slot, which):
        device, head = peer(slot)
        hbm, buf = kv[which]
        back = BACK[slot]
        return remote(
            hbm.at[:, columns(head, HD)],
            buf.at[0, 0, pl.ds(back * TOK, TOK), :],
            kv_out.at[which, slot], kv_in.at[which, back], device,
        )

    def q_copy(slot):
        device, head = peer(slot)
        back = BACK[slot]
        return remote(
            q_hbm.at[:, columns(head, RATIO * HD)],
            q_buf.at[back], q_out.at[slot], q_in.at[back], device,
        )

    def own_kv(which):
        hbm, buf = kv[which]
        return pltpu.make_async_copy(
            hbm.at[:, columns(my_head, HD)],
            buf.at[0, 0, pl.ds(0, TOK), :], kv_in.at[which, 0],
        )

    own_q = pltpu.make_async_copy(
        q_hbm.at[:, columns(my_head, RATIO * HD)], q_buf.at[0], q_in.at[0]
    )

    for which in range(2):
        own_kv(which).start()
    for slot in range(1, 8):
        for which in range(2):
            kv_copy(slot, which).start()
    own_q.start()
    for slot in range(1, 8):
        q_copy(slot).start()

    def piece(buf, seg, half, chunk):
        at = pl.multiple_of(chunk * CHUNK, CHUNK)
        return buf.at[seg, half, pl.ds(at, CHUNK), :]

    def own_to_sibling(which, chunk):
        buf = kv[which][1]
        return remote(
            piece(buf, 0, 0, chunk), piece(buf, 0, 1, chunk),
            own_out.at[which, chunk], own_in.at[which, chunk], sibling,
        )

    def hop(which, chunk):
        buf = kv[which][1]
        return remote(
            piece(buf, 0, 0, chunk), piece(buf, 1, 0, chunk),
            hop_out.at[which, chunk], hop_in.at[which, chunk], near,
        )

    def near_to_sibling(which, chunk):
        buf = kv[which][1]
        return remote(
            piece(buf, 1, 0, chunk), piece(buf, 1, 1, chunk),
            next_out.at[which, chunk], next_in.at[which, chunk], sibling,
        )

    def relay(which, chunk):
        buf = kv[which][1]
        return remote(
            piece(buf, 1, 0, chunk), piece(buf, 2, 0, chunk),
            relay_out.at[which, chunk], relay_in.at[which, chunk], onward,
        )

    def far_to_sibling(which):
        buf = kv[which][1]
        return remote(
            buf.at[2, 0], buf.at[2, 1], last_out.at[which], last_in.at[which], sibling
        )

    m_run[...] = jnp.full(m_run.shape, -jnp.inf, jnp.float32)
    for chunk in range(CHUNKS):
        for which in range(2):
            for slot in (2 * chunk, 2 * chunk + 1):
                if slot == 0:
                    own_kv(which).wait()
                else:
                    kv_copy(BACK[slot], which).wait_recv()
            own_to_sibling(which, chunk).start()
            hop(which, chunk).start()
    own_q.wait()

    def wait_q(slot):
        remote(
            q_hbm.at[:, columns(0, RATIO * HD)],
            q_buf.at[slot], q_out.at[slot], q_in.at[slot], sibling,
        ).wait_recv()

    def score(b, seg, side, floor=None, between=None):
        q = jnp.concatenate(
            [q_buf[b, :, h * HD : (h + 1) * HD] for h in range(RATIO)], axis=0
        )
        for kt in range(SEG // KT):
            half, at = divmod(kt * KT, HALF)
            if between is not None and kt * KT == HALF:
                between()
            s_buf[side, :, kt * KT : (kt + 1) * KT] = lax.dot_general(
                q, k_buf[seg, half, at : at + KT, :],
                (((1,), (1,)), ((), ())), preferred_element_type=jnp.float32,
            )
        for h in range(RATIO):
            r = slice(h * TOK, (h + 1) * TOK)
            top = s_buf[side, r, 0:HD]
            for j in range(1, SEG // HD):
                top = jnp.maximum(top, s_buf[side, r, j * HD : (j + 1) * HD])
            top = jnp.broadcast_to(jnp.max(top, axis=1, keepdims=True), (TOK, HD))
            if floor is not None:
                top = jnp.maximum(top, floor[r, :])
            m_cur[side, r, :] = top

    def mix(b, seg, side, last=False):
        m = m_cur[side]
        update = None
        for kt in range(SEG // KT):
            half, at = divmod(kt * KT, HALF)
            p = jnp.concatenate(
                [
                    jnp.exp2((s_buf[side, :, c : c + HD] - m) * SCALE).astype(jnp.bfloat16)
                    for c in range(kt * KT, (kt + 1) * KT, HD)
                ],
                axis=1,
            )
            wide = jnp.concatenate(
                [v_buf[seg, half, at : at + KT, :], jnp.ones((KT, HD), jnp.bfloat16)], axis=1
            )
            part = jnp.dot(p, wide, preferred_element_type=jnp.float32)
            update = part if update is None else update + part
        if seg:
            factor = jnp.exp2((m_run[b] - m) * SCALE)
            update = acc[b] * jnp.concatenate([factor, factor], axis=1) + update
        if last:
            finish(b, update)
        else:
            m_run[b] = m
            acc[b] = update

    def finish(b, total):
        mixed = (total[:, :HD] / total[:, HD:]).astype(jnp.bfloat16)
        for h in range(RATIO):
            o_buf[b, :, h * HD : (h + 1) * HD] = mixed[h * TOK : (h + 1) * TOK, :]

    def give(slot):
        device, head = peer(slot)
        return remote(
            o_buf.at[slot], o_hbm.at[:, columns(my_head, RATIO * HD)],
            o_out.at[slot], o_in.at[BACK[slot]], device,
        )

    own_o = pltpu.make_async_copy(
        o_buf.at[0], o_hbm.at[:, columns(my_head, RATIO * HD)], o_in.at[0]
    )

    def send_out(b):
        for slot in range(1, 8):
            pl.when(b == slot)(give(slot).start)

    def own_arrives():
        for chunk in range(CHUNKS):
            for which in range(2):
                own_to_sibling(which, chunk).wait_recv()

    def near_arrives(chunk):
        for which in range(2):
            hop(which, chunk).wait_recv()
            near_to_sibling(which, chunk).start()

        @pl.when(has_onward)
        def _():
            for which in range(2):
                relay(which, chunk).start()

    def far_arrives():
        for which in range(2):
            for chunk in range(CHUNKS):
                relay(which, chunk).wait_recv()
            far_to_sibling(which).start()
        for which in range(2):
            far_to_sibling(which).wait_recv()

    score(0, 0, 0, None, own_arrives)

    def own_pair(i, carry):
        b = 2 * i
        wait_q(b + 1)

        @pl.when(i >= 1)
        def _():
            near_arrives(i - 1)

        score(b + 1, 0, 1)
        mix(b, 0, 0)

        wait_q(b + 2)
        score(b + 2, 0, 0)
        mix(b + 1, 0, 1)
        return carry

    lax.fori_loop(0, 3, own_pair, 0)
    wait_q(7)
    near_arrives(2)
    score(7, 0, 1)
    mix(6, 0, 0)
    near_arrives(3)
    for chunk in range(CHUNKS):
        for which in range(2):
            near_to_sibling(which, chunk).wait_recv()
    score(7, 1, 0, m_cur.at[1])
    mix(7, 0, 1)

    @pl.when(has_far)
    def _():
        far_arrives()

        def both(t, carry):
            b = 7 - t
            score(b, 2, 1, m_cur.at[0])
            mix(b, 1, 0)
            score(b - 1, 1, 0, m_run.at[b - 1])
            mix(b, 2, 1, True)
            send_out(b)
            return carry

        lax.fori_loop(0, 7, both, 0)
        score(0, 2, 1, m_cur.at[0])
        mix(0, 1, 0)
        mix(0, 2, 1, True)
        own_o.start()

    @pl.when(no_far)
    def _():
        def single(i, carry):
            b = 7 - 2 * i
            score(b - 1, 1, 1, m_run.at[b - 1])
            mix(b, 1, 0, True)
            send_out(b)
            score(b - 2, 1, 0, m_run.at[b - 2])
            mix(b - 1, 1, 1, True)
            send_out(b - 1)
            return carry

        lax.fori_loop(0, 3, single, 0)
        score(0, 1, 1, m_run.at[0])
        mix(1, 1, 0, True)
        give(1).start()
        mix(0, 1, 1, True)
        own_o.start()

    for slot in range(1, 8):
        for which in range(2):
            kv_copy(slot, which).wait_send()
        q_copy(slot).wait_send()
    for which in range(2):
        for chunk in range(CHUNKS):
            own_to_sibling(which, chunk).wait_send()
            hop(which, chunk).wait_send()
            near_to_sibling(which, chunk).wait_send()

    @pl.when(has_onward)
    def _():
        for which in range(2):
            for chunk in range(CHUNKS):
                relay(which, chunk).wait_send()

    @pl.when(has_far)
    def _():
        for which in range(2):
            far_to_sibling(which).wait_send()

    own_o.wait()
    for slot in range(1, 8):
        device, head = peer(slot)
        give(slot).wait_send()
        remote(
            o_buf.at[slot], o_hbm.at[:, columns(head, RATIO * HD)],
            o_out.at[slot], o_in.at[slot], device,
        ).wait_recv()


def attention(queries, keys, values):
    dma = pltpu.SemaphoreType.DMA
    return pl.pallas_call(
        kernel,
        out_shape=jax.ShapeDtypeStruct(queries.shape, jnp.bfloat16),
        in_specs=[pl.BlockSpec(memory_space=pl.ANY)] * 3,
        out_specs=pl.BlockSpec(memory_space=pl.ANY),
        scratch_shapes=[
            pltpu.VMEM((8, TOK, RATIO * HD), jnp.bfloat16),
            pltpu.VMEM((3, 2, HALF, HD), jnp.bfloat16),
            pltpu.VMEM((3, 2, HALF, HD), jnp.bfloat16),
            pltpu.VMEM((8, TOK, RATIO * HD), jnp.bfloat16),
            pltpu.VMEM((2, ROWS, SEG), jnp.float32),
            pltpu.VMEM((2, ROWS, HD), jnp.float32),
            pltpu.VMEM((8, ROWS, HD), jnp.float32),
            pltpu.VMEM((8, ROWS, 2 * HD), jnp.float32),
            dma((8,)), dma((8,)),
            dma((2, 8)), dma((2, 8)),
            dma((2, CHUNKS)), dma((2, CHUNKS)),
            dma((2, CHUNKS)), dma((2, CHUNKS)),
            dma((2, CHUNKS)), dma((2, CHUNKS)),
            dma((2, CHUNKS)), dma((2, CHUNKS)),
            dma((2,)), dma((2,)),
            dma((8,)), dma((8,)),
        ],
        compiler_params=pltpu.CompilerParams(
            collective_id=0, has_side_effects=True, vmem_limit_bytes=58 * 2**20
        ),
        name="window_attention",
    )(queries, keys, values)


def solution(mesh):
    spec = P(("outer", "inner"), None)
    return jax.shard_map(
        attention, mesh=mesh, in_specs=(spec, spec, spec), out_specs=spec, check_vma=False
    )
```

```python
import jax
import jax.numpy as jnp
from jax import lax
from jax.experimental import pallas as pl
from jax.experimental.pallas import tpu as pltpu
from jax.sharding import PartitionSpec as P

QH = 32
KVH = 8
HD = 128
TOK = 128
RATIO = QH // KVH
ROWS = RATIO * TOK
HALF = 8 * TOK
SEG = 2 * HALF
KT = 256
SCALE = 1.4426950408889634 / HD**0.5
MESH = pl.DeviceIdType.MESH


STEPS = ((0, 0), (1, 0), (3, 0), (0, 1), (1, 1), (3, 1), (2, 0), (2, 1))
BACK = tuple(STEPS.index(((4 - dy) % 4, dz)) for dy, dz in STEPS)
CHUNKS = 4
CHUNK = HALF // CHUNKS


def kernel(
    q_hbm, k_hbm, v_hbm, o_hbm,
    q_buf, k_buf, v_buf, o_buf, s_buf, m_cur, m_run, acc,
    q_out, q_in, kv_out, kv_in, own_out, own_in, hop_out, hop_in,
    next_out, next_in, relay_out, relay_in, last_out, last_in, o_out, o_in,
):
    outer = lax.axis_index("outer")
    inner = lax.axis_index("inner")
    z_hi = outer % 2
    z_lo = inner // 8
    y = (inner // 2) % 4
    core = inner % 2
    kv = ((k_hbm, k_buf), (v_hbm, v_buf))

    def peer(slot):
        dy, dz = STEPS[slot]
        py = (y + dy) % 4
        pz = (z_lo + dz) % 2
        head = ((pz + z_hi) % 2) * 4 + py
        return (outer, pz * 8 + py * 2 + core), head

    def columns(head, width):
        return pl.ds(pl.multiple_of(head * width, width), width)

    my_head = ((z_lo + z_hi) % 2) * 4 + y
    sibling = (outer, inner + 1 - 2 * core)
    near = (outer + 1 - 2 * z_hi, (1 - z_lo) * 8 + y * 2 + core)
    onward_outer = outer + 2 - 4 * z_hi
    source_outer = outer - 2 + 4 * z_hi
    onward = (onward_outer, inner)
    source = (source_outer, inner)
    has_onward = jnp.logical_and(onward_outer >= 0, onward_outer < 8)
    has_far = jnp.logical_and(source_outer >= 0, source_outer < 8)
    no_far = jnp.logical_not(has_far)

    barrier = pltpu.get_barrier_semaphore()

    def greet(device):
        pl.semaphore_signal(barrier, inc=1, device_id=device, device_id_type=MESH)

    for slot in range(1, 8):
        greet(peer(slot)[0])
    greet(sibling)
    greet(near)

    @pl.when(has_onward)
    def _():
        greet(onward)

    @pl.when(has_far)
    def _():
        greet(source)

    inland = jnp.logical_and(has_onward, has_far)

    @pl.when(inland)
    def _():
        pl.semaphore_wait(barrier, 11)

    @pl.when(jnp.logical_not(inland))
    def _():
        pl.semaphore_wait(barrier, 10)

    def remote(src, dst, send, recv, device):
        return pltpu.make_async_remote_copy(
            src_ref=src, dst_ref=dst, send_sem=send, recv_sem=recv,
            device_id=device, device_id_type=MESH,
        )

    def kv_copy(slot, which):
        device, head = peer(slot)
        hbm, buf = kv[which]
        back = BACK[slot]
        return remote(
            hbm.at[:, columns(head, HD)],
            buf.at[0, 0, pl.ds(back * TOK, TOK), :],
            kv_out.at[which, slot], kv_in.at[which, back], device,
        )

    def q_copy(slot):
        device, head = peer(slot)
        back = BACK[slot]
        return remote(
            q_hbm.at[:, columns(head, RATIO * HD)],
            q_buf.at[back], q_out.at[slot], q_in.at[back], device,
        )

    def own_kv(which):
        hbm, buf = kv[which]
        return pltpu.make_async_copy(
            hbm.at[:, columns(my_head, HD)],
            buf.at[0, 0, pl.ds(0, TOK), :], kv_in.at[which, 0],
        )

    own_q = pltpu.make_async_copy(
        q_hbm.at[:, columns(my_head, RATIO * HD)], q_buf.at[0], q_in.at[0]
    )

    for which in range(2):
        own_kv(which).start()
    for slot in range(1, 8):
        for which in range(2):
            kv_copy(slot, which).start()
    own_q.start()
    for slot in range(1, 8):
        q_copy(slot).start()

    def piece(buf, seg, half, chunk):
        at = pl.multiple_of(chunk * CHUNK, CHUNK)
        return buf.at[seg, half, pl.ds(at, CHUNK), :]

    def own_to_sibling(which, chunk):
        buf = kv[which][1]
        return remote(
            piece(buf, 0, 0, chunk), piece(buf, 0, 1, chunk),
            own_out.at[which, chunk], own_in.at[which, chunk], sibling,
        )

    def hop(which, chunk):
        buf = kv[which][1]
        return remote(
            piece(buf, 0, 0, chunk), piece(buf, 1, 0, chunk),
            hop_out.at[which, chunk], hop_in.at[which, chunk], near,
        )

    def near_to_sibling(which, chunk):
        buf = kv[which][1]
        return remote(
            piece(buf, 1, 0, chunk), piece(buf, 1, 1, chunk),
            next_out.at[which, chunk], next_in.at[which, chunk], sibling,
        )

    def relay(which, chunk):
        buf = kv[which][1]
        return remote(
            piece(buf, 1, 0, chunk), piece(buf, 2, 0, chunk),
            relay_out.at[which, chunk], relay_in.at[which, chunk], onward,
        )

    def far_to_sibling(which):
        buf = kv[which][1]
        return remote(
            buf.at[2, 0], buf.at[2, 1], last_out.at[which], last_in.at[which], sibling
        )

    m_run[...] = jnp.full(m_run.shape, -jnp.inf, jnp.float32)
    for chunk in range(CHUNKS):
        for which in range(2):
            for slot in (2 * chunk, 2 * chunk + 1):
                if slot == 0:
                    own_kv(which).wait()
                else:
                    kv_copy(BACK[slot], which).wait_recv()
            own_to_sibling(which, chunk).start()
            hop(which, chunk).start()
    own_q.wait()

    def wait_q(slot):
        remote(
            q_hbm.at[:, columns(0, RATIO * HD)],
            q_buf.at[slot], q_out.at[slot], q_in.at[slot], sibling,
        ).wait_recv()

    def score(b, seg, side, floor=None, between=None):
        q = jnp.concatenate(
            [q_buf[b, :, h * HD : (h + 1) * HD] for h in range(RATIO)], axis=0
        )
        for kt in range(SEG // KT):
            half, at = divmod(kt * KT, HALF)
            if between is not None and kt * KT == HALF:
                between()
            s_buf[side, :, kt * KT : (kt + 1) * KT] = lax.dot_general(
                q, k_buf[seg, half, at : at + KT, :],
                (((1,), (1,)), ((), ())), preferred_element_type=jnp.float32,
            )
        for h in range(RATIO):
            r = slice(h * TOK, (h + 1) * TOK)
            top = s_buf[side, r, 0:HD]
            for j in range(1, SEG // HD):
                top = jnp.maximum(top, s_buf[side, r, j * HD : (j + 1) * HD])
            top = jnp.broadcast_to(jnp.max(top, axis=1, keepdims=True), (TOK, HD))
            if floor is not None:
                top = jnp.maximum(top, floor[r, :])
            m_cur[side, r, :] = top

    def mix(b, seg, side, last=False):
        m = m_cur[side]
        update = None
        for kt in range(SEG // KT):
            half, at = divmod(kt * KT, HALF)
            p = jnp.concatenate(
                [
                    jnp.exp2((s_buf[side, :, c : c + HD] - m) * SCALE).astype(jnp.bfloat16)
                    for c in range(kt * KT, (kt + 1) * KT, HD)
                ],
                axis=1,
            )
            wide = jnp.concatenate(
                [v_buf[seg, half, at : at + KT, :], jnp.ones((KT, HD), jnp.bfloat16)], axis=1
            )
            part = jnp.dot(p, wide, preferred_element_type=jnp.float32)
            update = part if update is None else update + part
        if seg:
            factor = jnp.exp2((m_run[b] - m) * SCALE)
            update = acc[b] * jnp.concatenate([factor, factor], axis=1) + update
        if last:
            finish(b, update)
        else:
            m_run[b] = m
            acc[b] = update

    def finish(b, total):
        mixed = (total[:, :HD] / total[:, HD:]).astype(jnp.bfloat16)
        for h in range(RATIO):
            o_buf[b, :, h * HD : (h + 1) * HD] = mixed[h * TOK : (h + 1) * TOK, :]

    def give(slot):
        device, head = peer(slot)
        return remote(
            o_buf.at[slot], o_hbm.at[:, columns(my_head, RATIO * HD)],
            o_out.at[slot], o_in.at[BACK[slot]], device,
        )

    own_o = pltpu.make_async_copy(
        o_buf.at[0], o_hbm.at[:, columns(my_head, RATIO * HD)], o_in.at[0]
    )

    def send_out(b):
        for slot in range(1, 8):
            pl.when(b == slot)(give(slot).start)

    def own_arrives():
        for chunk in range(CHUNKS):
            for which in range(2):
                own_to_sibling(which, chunk).wait_recv()

    def near_arrives(chunk):
        for which in range(2):
            hop(which, chunk).wait_recv()
            near_to_sibling(which, chunk).start()

        @pl.when(has_onward)
        def _():
            for which in range(2):
                relay(which, chunk).start()

    def far_arrives():
        for which in range(2):
            for chunk in range(CHUNKS):
                relay(which, chunk).wait_recv()
            far_to_sibling(which).start()

    score(0, 0, 0, None, own_arrives)

    def own_pair(i, carry):
        b = 2 * i
        wait_q(b + 1)

        @pl.when(i >= 1)
        def _():
            near_arrives(i - 1)

        score(b + 1, 0, 1)
        mix(b, 0, 0)

        wait_q(b + 2)
        score(b + 2, 0, 0)
        mix(b + 1, 0, 1)
        return carry

    lax.fori_loop(0, 3, own_pair, 0)
    wait_q(7)
    near_arrives(2)
    score(7, 0, 1)
    mix(6, 0, 0)
    near_arrives(3)
    for chunk in range(CHUNKS):
        for which in range(2):
            near_to_sibling(which, chunk).wait_recv()
    score(7, 1, 0, m_cur.at[1])
    mix(7, 0, 1)

    @pl.when(has_far)
    def _():
        def near_pair(i, carry):
            b = 7 - 2 * i

            @pl.when(i == 2)
            def _():
                far_arrives()

            score(b - 1, 1, 1, m_run.at[b - 1])
            mix(b, 1, 0)

            @pl.when(i == 2)
            def _():
                for which in range(2):
                    far_to_sibling(which).wait_recv()

            then = i // 2
            score(b - 2 + 6 * then, 1 + then, 0, m_run.at[b - 2 + 6 * then])
            mix(b - 1, 1, 1)
            return carry

        lax.fori_loop(0, 3, near_pair, 0)

        def far_pair(i, carry):
            b = 7 - 2 * i
            score(b - 1, 2, 1, m_run.at[b - 1])
            mix(b, 2, 0, True)
            send_out(b)
            score(b - 2, 2 - i // 2, 0, m_run.at[b - 2])
            mix(b - 1, 2, 1, True)
            send_out(b - 1)
            return carry

        lax.fori_loop(0, 3, far_pair, 0)
        score(1, 2, 1, m_cur.at[0])
        mix(1, 1, 0)
        score(0, 1, 0, m_run.at[0])
        mix(1, 2, 1, True)
        give(1).start()
        score(0, 2, 1, m_cur.at[0])
        mix(0, 1, 0)
        mix(0, 2, 1, True)
        own_o.start()

    @pl.when(no_far)
    def _():
        def single(i, carry):
            b = 7 - 2 * i
            score(b - 1, 1, 1, m_run.at[b - 1])
            mix(b, 1, 0, True)
            send_out(b)
            score(b - 2, 1, 0, m_run.at[b - 2])
            mix(b - 1, 1, 1, True)
            send_out(b - 1)
            return carry

        lax.fori_loop(0, 3, single, 0)
        score(0, 1, 1, m_run.at[0])
        mix(1, 1, 0, True)
        give(1).start()
        mix(0, 1, 1, True)
        own_o.start()

    for slot in range(1, 8):
        for which in range(2):
            kv_copy(slot, which).wait_send()
        q_copy(slot).wait_send()
    for which in range(2):
        for chunk in range(CHUNKS):
            own_to_sibling(which, chunk).wait_send()
            hop(which, chunk).wait_send()
            near_to_sibling(which, chunk).wait_send()

    @pl.when(has_onward)
    def _():
        for which in range(2):
            for chunk in range(CHUNKS):
                relay(which, chunk).wait_send()

    @pl.when(has_far)
    def _():
        for which in range(2):
            far_to_sibling(which).wait_send()

    own_o.wait()
    for slot in range(1, 8):
        device, head = peer(slot)
        give(slot).wait_send()
        remote(
            o_buf.at[slot], o_hbm.at[:, columns(head, RATIO * HD)],
            o_out.at[slot], o_in.at[slot], device,
        ).wait_recv()


def attention(queries, keys, values):
    dma = pltpu.SemaphoreType.DMA
    return pl.pallas_call(
        kernel,
        out_shape=jax.ShapeDtypeStruct(queries.shape, jnp.bfloat16),
        in_specs=[pl.BlockSpec(memory_space=pl.ANY)] * 3,
        out_specs=pl.BlockSpec(memory_space=pl.ANY),
        scratch_shapes=[
            pltpu.VMEM((8, TOK, RATIO * HD), jnp.bfloat16),
            pltpu.VMEM((3, 2, HALF, HD), jnp.bfloat16),
            pltpu.VMEM((3, 2, HALF, HD), jnp.bfloat16),
            pltpu.VMEM((8, TOK, RATIO * HD), jnp.bfloat16),
            pltpu.VMEM((2, ROWS, SEG), jnp.float32),
            pltpu.VMEM((2, ROWS, HD), jnp.float32),
            pltpu.VMEM((8, ROWS, HD), jnp.float32),
            pltpu.VMEM((8, ROWS, 2 * HD), jnp.float32),
            dma((8,)), dma((8,)),
            dma((2, 8)), dma((2, 8)),
            dma((2, CHUNKS)), dma((2, CHUNKS)),
            dma((2, CHUNKS)), dma((2, CHUNKS)),
            dma((2, CHUNKS)), dma((2, CHUNKS)),
            dma((2, CHUNKS)), dma((2, CHUNKS)),
            dma((2,)), dma((2,)),
            dma((8,)), dma((8,)),
        ],
        compiler_params=pltpu.CompilerParams(
            collective_id=0, has_side_effects=True, vmem_limit_bytes=30 * 2**20
        ),
        name="window_attention",
    )(*(pltpu.with_memory_space_constraint(a, pltpu.HBM) for a in (queries, keys, values)))


def solution(mesh):
    spec = P(("outer", "inner"), None)
    return jax.shard_map(
        attention, mesh=mesh, in_specs=(spec, spec, spec), out_specs=spec, check_vma=False
    )
```

```python
import jax
import jax.numpy as jnp
from jax import lax
from jax.experimental import pallas as pl
from jax.experimental.pallas import tpu as pltpu
from jax.sharding import PartitionSpec as P

QH = 32
KVH = 8
HD = 128
TOK = 128
RATIO = QH // KVH
ROWS = RATIO * TOK
HALF = 8 * TOK
SEG = 2 * HALF
KT = 256
SCALE = 1.4426950408889634 / HD**0.5
MESH = pl.DeviceIdType.MESH


STEPS = ((0, 0), (1, 0), (3, 0), (0, 1), (1, 1), (3, 1), (2, 0), (2, 1))
BACK = tuple(STEPS.index(((4 - dy) % 4, dz)) for dy, dz in STEPS)
CHUNKS = 4
CHUNK = HALF // CHUNKS


def kernel(
    q_hbm, k_hbm, v_hbm, o_hbm,
    q_buf, k_buf, v_buf, o_buf, s_buf, m_cur, m_run, acc,
    q_out, q_in, kv_out, kv_in, own_out, own_in, hop_out, hop_in,
    next_out, next_in, relay_out, relay_in, last_out, last_in, o_out, o_in,
):
    outer = lax.axis_index("outer")
    inner = lax.axis_index("inner")
    z_hi = outer % 2
    z_lo = inner // 8
    y = (inner // 2) % 4
    core = inner % 2
    kv = ((k_hbm, k_buf), (v_hbm, v_buf))

    def peer(slot):
        dy, dz = STEPS[slot]
        py = (y + dy) % 4
        pz = (z_lo + dz) % 2
        head = ((pz + z_hi) % 2) * 4 + py
        return (outer, pz * 8 + py * 2 + core), head

    def columns(head, width):
        return pl.ds(pl.multiple_of(head * width, width), width)

    my_head = ((z_lo + z_hi) % 2) * 4 + y
    sibling = (outer, inner + 1 - 2 * core)
    near = (outer + 1 - 2 * z_hi, (1 - z_lo) * 8 + y * 2 + core)
    onward_outer = outer + 2 - 4 * z_hi
    source_outer = outer - 2 + 4 * z_hi
    onward = (onward_outer, inner)
    source = (source_outer, inner)
    has_onward = jnp.logical_and(onward_outer >= 0, onward_outer < 8)
    has_far = jnp.logical_and(source_outer >= 0, source_outer < 8)
    no_far = jnp.logical_not(has_far)

    barrier = pltpu.get_barrier_semaphore()

    def greet(device):
        pl.semaphore_signal(barrier, inc=1, device_id=device, device_id_type=MESH)

    for slot in range(1, 8):
        greet(peer(slot)[0])
    greet(sibling)
    greet(near)

    @pl.when(has_onward)
    def _():
        greet(onward)

    @pl.when(has_far)
    def _():
        greet(source)

    inland = jnp.logical_and(has_onward, has_far)

    @pl.when(inland)
    def _():
        pl.semaphore_wait(barrier, 11)

    @pl.when(jnp.logical_not(inland))
    def _():
        pl.semaphore_wait(barrier, 10)

    def remote(src, dst, send, recv, device):
        return pltpu.make_async_remote_copy(
            src_ref=src, dst_ref=dst, send_sem=send, recv_sem=recv,
            device_id=device, device_id_type=MESH,
        )

    def kv_copy(slot, which):
        device, head = peer(slot)
        hbm, buf = kv[which]
        back = BACK[slot]
        return remote(
            hbm.at[:, columns(head, HD)],
            buf.at[0, 0, pl.ds(back * TOK, TOK), :],
            kv_out.at[which, slot], kv_in.at[which, back], device,
        )

    def q_copy(slot):
        device, head = peer(slot)
        back = BACK[slot]
        return remote(
            q_hbm.at[:, columns(head, RATIO * HD)],
            q_buf.at[back], q_out.at[slot], q_in.at[back], device,
        )

    def own_kv(which):
        hbm, buf = kv[which]
        return pltpu.make_async_copy(
            hbm.at[:, columns(my_head, HD)],
            buf.at[0, 0, pl.ds(0, TOK), :], kv_in.at[which, 0],
        )

    own_q = pltpu.make_async_copy(
        q_hbm.at[:, columns(my_head, RATIO * HD)], q_buf.at[0], q_in.at[0]
    )

    for which in range(2):
        own_kv(which).start()
    for slot in range(1, 8):
        for which in range(2):
            kv_copy(slot, which).start()
    own_q.start()
    for slot in range(1, 8):
        q_copy(slot).start()

    def piece(buf, seg, half, chunk):
        at = pl.multiple_of(chunk * CHUNK, CHUNK)
        return buf.at[seg, half, pl.ds(at, CHUNK), :]

    def own_to_sibling(which, chunk):
        buf = kv[which][1]
        return remote(
            piece(buf, 0, 0, chunk), piece(buf, 0, 1, chunk),
            own_out.at[which, chunk], own_in.at[which, chunk], sibling,
        )

    def hop(which, chunk):
        buf = kv[which][1]
        return remote(
            piece(buf, 0, 0, chunk), piece(buf, 1, 0, chunk),
            hop_out.at[which, chunk], hop_in.at[which, chunk], near,
        )

    def near_to_sibling(which, chunk):
        buf = kv[which][1]
        return remote(
            piece(buf, 1, 0, chunk), piece(buf, 1, 1, chunk),
            next_out.at[which, chunk], next_in.at[which, chunk], sibling,
        )

    def relay(which, chunk):
        buf = kv[which][1]
        return remote(
            piece(buf, 1, 0, chunk), piece(buf, 2, 0, chunk),
            relay_out.at[which, chunk], relay_in.at[which, chunk], onward,
        )

    def far_to_sibling(which):
        buf = kv[which][1]
        return remote(
            buf.at[2, 0], buf.at[2, 1], last_out.at[which], last_in.at[which], sibling
        )

    m_run[...] = jnp.full(m_run.shape, -jnp.inf, jnp.float32)
    for chunk in range(CHUNKS):
        for which in range(2):
            for slot in (2 * chunk, 2 * chunk + 1):
                if slot == 0:
                    own_kv(which).wait()
                else:
                    kv_copy(BACK[slot], which).wait_recv()
            own_to_sibling(which, chunk).start()
            hop(which, chunk).start()
    own_q.wait()

    def wait_q(slot):
        remote(
            q_hbm.at[:, columns(0, RATIO * HD)],
            q_buf.at[slot], q_out.at[slot], q_in.at[slot], sibling,
        ).wait_recv()

    def score(b, seg, side, floor=None, between=None):
        q = jnp.concatenate(
            [q_buf[b, :, h * HD : (h + 1) * HD] for h in range(RATIO)], axis=0
        )
        for kt in range(SEG // KT):
            half, at = divmod(kt * KT, HALF)
            if between is not None and kt * KT == HALF:
                between()
            s_buf[side, :, kt * KT : (kt + 1) * KT] = lax.dot_general(
                q, k_buf[seg, half, at : at + KT, :],
                (((1,), (1,)), ((), ())), preferred_element_type=jnp.float32,
            )
        for h in range(RATIO):
            r = slice(h * TOK, (h + 1) * TOK)
            top = s_buf[side, r, 0:HD]
            for j in range(1, SEG // HD):
                top = jnp.maximum(top, s_buf[side, r, j * HD : (j + 1) * HD])
            top = jnp.broadcast_to(jnp.max(top, axis=1, keepdims=True), (TOK, HD))
            if floor is not None:
                top = jnp.maximum(top, floor[r, :])
            m_cur[side, r, :] = top

    def mix(b, seg, side, last=False):
        m = m_cur[side]
        update = None
        for kt in range(SEG // KT):
            half, at = divmod(kt * KT, HALF)
            p = jnp.concatenate(
                [
                    jnp.exp2((s_buf[side, :, c : c + HD] - m) * SCALE).astype(jnp.bfloat16)
                    for c in range(kt * KT, (kt + 1) * KT, HD)
                ],
                axis=1,
            )
            wide = jnp.concatenate(
                [v_buf[seg, half, at : at + KT, :], jnp.ones((KT, HD), jnp.bfloat16)], axis=1
            )
            part = jnp.dot(p, wide, preferred_element_type=jnp.float32)
            update = part if update is None else update + part
        if seg:
            factor = jnp.exp2((m_run[b] - m) * SCALE)
            update = acc[b] * jnp.concatenate([factor, factor], axis=1) + update
        if last:
            finish(b, update)
        else:
            m_run[b] = m
            acc[b] = update

    def finish(b, total):
        mixed = (total[:, :HD] / total[:, HD:]).astype(jnp.bfloat16)
        for h in range(RATIO):
            o_buf[b, :, h * HD : (h + 1) * HD] = mixed[h * TOK : (h + 1) * TOK, :]

    def give(slot):
        device, head = peer(slot)
        return remote(
            o_buf.at[slot], o_hbm.at[:, columns(my_head, RATIO * HD)],
            o_out.at[slot], o_in.at[BACK[slot]], device,
        )

    own_o = pltpu.make_async_copy(
        o_buf.at[0], o_hbm.at[:, columns(my_head, RATIO * HD)], o_in.at[0]
    )

    def send_out(b):
        for slot in range(1, 8):
            pl.when(b == slot)(give(slot).start)

    def own_arrives():
        for chunk in range(CHUNKS):
            for which in range(2):
                own_to_sibling(which, chunk).wait_recv()

    def near_arrives(chunk):
        for which in range(2):
            hop(which, chunk).wait_recv()
            near_to_sibling(which, chunk).start()

        @pl.when(has_onward)
        def _():
            for which in range(2):
                relay(which, chunk).start()

    def far_arrives():
        for which in range(2):
            for chunk in range(CHUNKS):
                relay(which, chunk).wait_recv()
            far_to_sibling(which).start()

    score(0, 0, 0, None, own_arrives)

    def own_pair(i, carry):
        b = 2 * i
        wait_q(b + 1)

        @pl.when(i >= 1)
        def _():
            near_arrives(i - 1)

        score(b + 1, 0, 1)
        mix(b, 0, 0)

        wait_q(b + 2)
        score(b + 2, 0, 0)
        mix(b + 1, 0, 1)
        return carry

    lax.fori_loop(0, 3, own_pair, 0)
    wait_q(7)
    near_arrives(2)
    near_arrives(3)
    score(7, 0, 1)
    mix(6, 0, 0)
    for chunk in range(CHUNKS):
        for which in range(2):
            near_to_sibling(which, chunk).wait_recv()
    score(7, 1, 0, m_cur.at[1])
    mix(7, 0, 1)

    @pl.when(has_far)
    def _():
        def near_pair(i, carry):
            b = 7 - 2 * i

            score(b - 1, 1, 1, m_run.at[b - 1])
            mix(b, 1, 0)
            pl.when(i == 1)(far_arrives)

            @pl.when(i == 2)
            def _():
                for which in range(2):
                    far_to_sibling(which).wait_recv()

            then = i // 2
            score(b - 2 + 6 * then, 1 + then, 0, m_run.at[b - 2 + 6 * then])
            mix(b - 1, 1, 1)
            return carry

        lax.fori_loop(0, 3, near_pair, 0)

        def far_pair(i, carry):
            b = 7 - 2 * i
            score(b - 1, 2, 1, m_run.at[b - 1])
            mix(b, 2, 0, True)
            send_out(b)
            score(b - 2, 2 - i // 2, 0, m_run.at[b - 2])
            mix(b - 1, 2, 1, True)
            send_out(b - 1)
            return carry

        lax.fori_loop(0, 3, far_pair, 0)
        score(1, 2, 1, m_cur.at[0])
        mix(1, 1, 0)
        score(0, 1, 0, m_run.at[0])
        mix(1, 2, 1, True)
        give(1).start()
        score(0, 2, 1, m_cur.at[0])
        mix(0, 1, 0)
        mix(0, 2, 1, True)
        own_o.start()

    @pl.when(no_far)
    def _():
        def single(i, carry):
            b = 7 - 2 * i
            score(b - 1, 1, 1, m_run.at[b - 1])
            mix(b, 1, 0, True)
            send_out(b)
            score(b - 2, 1, 0, m_run.at[b - 2])
            mix(b - 1, 1, 1, True)
            send_out(b - 1)
            return carry

        lax.fori_loop(0, 3, single, 0)
        score(0, 1, 1, m_run.at[0])
        mix(1, 1, 0, True)
        give(1).start()
        mix(0, 1, 1, True)
        own_o.start()

    for slot in range(1, 8):
        for which in range(2):
            kv_copy(slot, which).wait_send()
        q_copy(slot).wait_send()
    for which in range(2):
        for chunk in range(CHUNKS):
            own_to_sibling(which, chunk).wait_send()
            hop(which, chunk).wait_send()
            near_to_sibling(which, chunk).wait_send()

    @pl.when(has_onward)
    def _():
        for which in range(2):
            for chunk in range(CHUNKS):
                relay(which, chunk).wait_send()

    @pl.when(has_far)
    def _():
        for which in range(2):
            far_to_sibling(which).wait_send()

    own_o.wait()
    for slot in range(1, 8):
        device, head = peer(slot)
        give(slot).wait_send()
        remote(
            o_buf.at[slot], o_hbm.at[:, columns(head, RATIO * HD)],
            o_out.at[slot], o_in.at[slot], device,
        ).wait_recv()


def attention(queries, keys, values):
    dma = pltpu.SemaphoreType.DMA
    return pl.pallas_call(
        kernel,
        out_shape=jax.ShapeDtypeStruct(queries.shape, jnp.bfloat16),
        in_specs=[pl.BlockSpec(memory_space=pl.ANY)] * 3,
        out_specs=pl.BlockSpec(memory_space=pl.ANY),
        scratch_shapes=[
            pltpu.VMEM((8, TOK, RATIO * HD), jnp.bfloat16),
            pltpu.VMEM((3, 2, HALF, HD), jnp.bfloat16),
            pltpu.VMEM((3, 2, HALF, HD), jnp.bfloat16),
            pltpu.VMEM((8, TOK, RATIO * HD), jnp.bfloat16),
            pltpu.VMEM((2, ROWS, SEG), jnp.float32),
            pltpu.VMEM((2, ROWS, HD), jnp.float32),
            pltpu.VMEM((8, ROWS, HD), jnp.float32),
            pltpu.VMEM((8, ROWS, 2 * HD), jnp.float32),
            dma((8,)), dma((8,)),
            dma((2, 8)), dma((2, 8)),
            dma((2, CHUNKS)), dma((2, CHUNKS)),
            dma((2, CHUNKS)), dma((2, CHUNKS)),
            dma((2, CHUNKS)), dma((2, CHUNKS)),
            dma((2, CHUNKS)), dma((2, CHUNKS)),
            dma((2,)), dma((2,)),
            dma((8,)), dma((8,)),
        ],
        compiler_params=pltpu.CompilerParams(
            collective_id=0, has_side_effects=True, vmem_limit_bytes=30 * 2**20
        ),
        name="window_attention",
    )(*(pltpu.with_memory_space_constraint(a, pltpu.HBM) for a in (queries, keys, values)))


def solution(mesh):
    spec = P(("outer", "inner"), None)
    return jax.shard_map(
        attention, mesh=mesh, in_specs=(spec, spec, spec), out_specs=spec, check_vma=False
    )
```
